32 devices in a mesh: gz: 32 (over z, y, x, core).
Axes of the slice: x: 2, y: 2, z: 4, core: 2. Of those that a mesh axis runs over, the one named last changes fastest.
Arguments:
- right_side: float32 [64, 512, 512], P('gz'), may hold values from -20 to 20
- cell_flags: int32 [64, 512, 512], P('gz'), may hold values from 0 to 2
Outputs:
- solution: float32 [64, 512, 512], P('gz')
- residual: float32 [64, 512, 512], P('gz')
The draws below stay inside these ranges and needn't reach their ends.
All inputs are finite; a program needn't handle non-finite values.
Results may differ from the reference program's by a relative error of at most 0.00011.
Values sent between devices are 32-bit elements; how exact they have to be, the bound alone decides.
A program may use at most 128 MiB of HBM per device.

```python
import math
import jax
import jax.numpy as jnp

NX = 512
NY = 512
ITERS = 2
NZ = 64


def draw_right_side(key, part):
    noise_key, phase_key = jax.random.split(key)
    depth = jnp.arange(NZ, dtype=jnp.float32) / max(NZ - 1, 1)
    across = (jnp.arange(NX, dtype=jnp.float32) + 0.5) / NX
    along = (jnp.arange(NY, dtype=jnp.float32) + 0.5) / NY
    phases = jax.random.uniform(phase_key, (2,), jnp.float32, 0.0, 2.0 * math.pi)
    base = jnp.clip(jax.random.normal(noise_key, (NZ, NX, NY), jnp.float32), -6.0, 6.0)
    wave = jnp.cos(2.0 * math.pi * across + phases[0])[:, None] * jnp.cos(2.0 * math.pi * along + phases[1])[None, :]
    upper_weight = 3.0 * depth * depth
    return base + upper_weight[:, None, None] * wave[None, :, :]


def draw_cell_flags(key, part):
    keys = jax.random.split(key, 9)
    block_z = max(NZ // 16, 2)
    block_x = max(NX // 8, 4)
    block_y = max(NY // 8, 4)
    count_z = (NZ + block_z - 1) // block_z
    count_x = (NX + block_x - 1) // block_x
    count_y = (NY + block_y - 1) // block_y
    blocks = (count_z, count_x, count_y)
    level = jnp.arange(count_z, dtype=jnp.int32)[:, None, None]
    present = jax.random.randint(keys[0], blocks, 0, count_z) >= level

    def extent(length_key, start_key, width):
        shortest = max(width // 3, 1)
        longest = max(2 * width // 3, shortest)
        length = jax.random.randint(length_key, blocks, shortest, longest + 1)
        start = jax.random.randint(start_key, blocks, 0, width - length + 1)
        return (start, length)
    start_z, length_z = extent(keys[1], keys[2], block_z)
    start_x, length_x = extent(keys[3], keys[4], block_x)
    start_y, length_y = extent(keys[5], keys[6], block_y)
    zcells = jnp.arange(NZ, dtype=jnp.int32)
    xcells = jnp.arange(NX, dtype=jnp.int32)
    ycells = jnp.arange(NY, dtype=jnp.int32)
    z_index = (zcells // block_z)[:, None, None]
    x_index = (xcells // block_x)[None, :, None]
    y_index = (ycells // block_y)[None, None, :]
    z_offset = (zcells % block_z)[:, None, None]
    x_offset = (xcells % block_x)[None, :, None]
    y_offset = (ycells % block_y)[None, None, :]

    def inside(start, length, offset):
        first = start[z_index, x_index, y_index]
        return (offset >= first) & (offset < first + length[z_index, x_index, y_index])
    solid = present[z_index, x_index, y_index] & inside(start_z, length_z, z_offset) & inside(start_x, length_x, x_offset) & inside(start_y, length_y, y_offset)
    scattered = jax.random.randint(keys[8], (NZ, NX, NY), 0, 8) == 0
    solid = solid | scattered
    edge_draw = jax.random.randint(keys[7], (NZ, 2, NY), 0, 4) == 0
    open_edge = jnp.pad(edge_draw, ((0, 0), (0, NX - 2), (0, 0)))
    open_side = (ycells >= NY - 2)[None, None, :]
    empty = open_edge | open_side
    return jnp.where(solid, 2, jnp.where(empty, 0, 1)).astype(jnp.int32)


def setup_inputs(seed: int = 0) -> dict:
    key_of = jax.random.split(jax.random.key(seed), 3)
    right_side = draw_right_side(jax.random.fold_in(key_of[2], 71), 0)
    cell_flags = draw_cell_flags(jax.random.fold_in(key_of[2], 71), 0)
    return dict(right_side=right_side, cell_flags=cell_flags)


def neighbour_total(field):
    padded = jnp.pad(field, 1)
    total = padded[2:, 1:-1, 1:-1] + padded[:-2, 1:-1, 1:-1]
    total = total + padded[1:-1, 2:, 1:-1] + padded[1:-1, :-2, 1:-1]
    total = total + padded[1:-1, 1:-1, 2:] + padded[1:-1, 1:-1, :-2]
    return total


def reference(right_side, cell_flags):
    fluid_mask = (cell_flags == 1).astype(jnp.float32)
    solid = (cell_flags == 2).astype(jnp.float32)
    diagonal = jnp.maximum(6.0 - neighbour_total(solid), 1.0)

    def operate(field):
        return fluid_mask * (diagonal * field - neighbour_total(field))

    solution = jnp.zeros_like(right_side)
    residual = fluid_mask * right_side
    precond = residual / diagonal
    direction = precond
    rz_now = jnp.sum(residual * precond)
    for iteration in range(ITERS):
        image = operate(direction)
        step_size = rz_now / jnp.sum(direction * image)
        solution = solution + step_size * direction
        residual = residual - step_size * image
        if iteration + 1 < ITERS:
            precond = residual / diagonal
            rz_new = jnp.sum(residual * precond)
            direction = precond + (rz_new / rz_now) * direction
            rz_now = rz_new
    return solution, residual
```

```python
import functools
import math

import jax
import jax.numpy as jnp
from jax import lax
from jax.experimental import pallas as pl
from jax.experimental.pallas import tpu as pltpu
from jax.sharding import PartitionSpec as P

MESH = pl.DeviceIdType.MESH
TILE = 16
PAD = 8


def kernel(
    count, near, chunk,
    side_hbm, flag_hbm, sol_hbm, res_hbm,
    rhs, flags, r0, inv, solid, u0, u1, w0, w1, halo_r, halo_u, bits_out, bits_in,
    mine, near_got, far_got,
    in_sem, out_sem, bit_send, bit_recv, halo_send, halo_recv,
    near_send, near_recv, far_send, far_recv,
):
    depth, rows, cols = rhs.shape
    words = rows // 32
    chunks = rows // chunk
    tiles = chunk // TILE
    far = count // near
    me = lax.axis_index("gz")
    low, high = lax.rem(me, near), me // near
    first_side = 1 - lax.rem(me, 2)

    def load(plane, which):
        source, target = ((flag_hbm, flags), (side_hbm, rhs))[which]
        return pltpu.make_async_copy(source.at[plane], target.at[plane], in_sem.at[which, plane])

    for plane in range(depth):
        for which in range(2):
            load(plane, which).start()

    def present(side):
        return jnp.where(side == 0, me > 0, me < count - 1)

    def neighbour(side):
        return me - 1 + 2 * side

    near_ids = [high * near + lax.rem(low + j, near) for j in range(1, near)]
    far_ids = [lax.rem(high + j, far) * near + low for j in range(1, far)]
    barrier = pltpu.get_barrier_semaphore()
    for other in near_ids + far_ids:
        pl.semaphore_signal(barrier, inc=1, device_id=(other,), device_id_type=MESH)
    outside = (
        jnp.logical_and(low == 0, me > 0),
        jnp.logical_and(low == near - 1, me < count - 1),
    )
    for side in range(2):
        @pl.when(outside[side])
        def _():
            pl.semaphore_signal(barrier, inc=1, device_id=(neighbour(side),), device_id_type=MESH)

    blank = jnp.zeros((PAD, cols), jnp.float32)
    for ref in (u0, u1, solid):
        for plane in range(ref.shape[0]):
            ref[plane, 0:PAD, :] = blank
            ref[plane, rows + PAD:rows + 2 * PAD, :] = blank
    for side in range(2):
        @pl.when(jnp.logical_not(present(side)))
        def _():
            bits_in[side] = jnp.zeros((2, words, cols), jnp.int32)

            def clear(t, carry):
                at = pl.ds(pl.multiple_of(t * TILE, TILE), TILE)
                halo_r[side, at, :] = jnp.zeros((TILE, cols), jnp.float32)
                halo_u[side, at, :] = jnp.zeros((TILE, cols), jnp.float32)
                return carry

            lax.fori_loop(0, rows // TILE, clear, 0)

    outer = sorted({0, 1, depth - 2, depth - 1})
    for plane in range(depth):
        load(plane, 0).wait()

        def pack(j, word, plane=plane):
            at = pl.ds(pl.multiple_of(j * words, words), words)
            is_solid = flags[plane, at, :] == 2
            padded = pl.ds(pl.multiple_of(j * words + PAD, PAD), words)
            solid[plane + 2, padded, :] = jnp.where(is_solid, 1.0, 0.0)
            return word | jnp.left_shift(jnp.where(is_solid, 1, 0), j)

        word = lax.fori_loop(0, 32, pack, jnp.zeros((words, cols), jnp.int32))
        if plane in outer:
            bits_out[outer.index(plane)] = word

    peers = near + far - 2 + outside[0].astype(jnp.int32) + outside[1].astype(jnp.int32)
    pl.semaphore_wait(barrier, peers)

    def bit_copy(side):
        lead = 0 if side == 0 else len(outer) - 2
        return pltpu.make_async_remote_copy(
            src_ref=bits_out.at[pl.ds(lead, 2)],
            dst_ref=bits_in.at[1 - side],
            send_sem=bit_send.at[side],
            recv_sem=bit_recv.at[1 - side],
            device_id=(neighbour(side),),
            device_id_type=MESH,
        )

    for side in range(2):
        @pl.when(present(side))
        def _():
            bit_copy(side).start()

    def halo_copy(phase, side, k):
        at = pl.multiple_of(k * chunk, chunk)
        plane = side * (depth - 1)
        if phase == 0:
            source, target = r0.at[plane, pl.ds(at, chunk)], halo_r
        else:
            source, target = u1.at[plane, pl.ds(pl.multiple_of(at + PAD, PAD), chunk)], halo_u
        return pltpu.make_async_remote_copy(
            src_ref=source,
            dst_ref=target.at[1 - side, pl.ds(at, chunk)],
            send_sem=halo_send.at[phase, side, k],
            recv_sem=halo_recv.at[phase, 1 - side, k],
            device_id=(neighbour(side),),
            device_id_type=MESH,
        )

    def halo_arrival(phase, side, k):
        at = pl.multiple_of(k * chunk, chunk)
        target = halo_r if phase == 0 else halo_u
        return pltpu.make_async_remote_copy(
            src_ref=target.at[side, pl.ds(at, chunk)],
            dst_ref=target.at[side, pl.ds(at, chunk)],
            send_sem=halo_send.at[phase, side, k],
            recv_sem=halo_recv.at[phase, side, k],
            device_id=(neighbour(side),),
            device_id_type=MESH,
        )

    def send_halo(phase, side, k):
        @pl.when(present(side))
        def _():
            halo_copy(phase, side, k).start()

    def wait_halo(phase, side, k):
        @pl.when(present(side))
        def _():
            halo_arrival(phase, side, k).wait_recv()

    def row(k, t):
        return pl.multiple_of(k * chunk + t * TILE, TILE)

    for plane in range(depth):
        load(plane, 1).wait()
    edge_first = [0, depth - 1] + list(range(1, depth - 1))

    def mask_chunk(k, carry):
        for plane in edge_first:
            def mask_tile(t, carry, plane=plane):
                at = pl.ds(row(k, t), TILE)
                r0[plane, at, :] = jnp.where(flags[plane, at, :] == 1, rhs[plane, at, :], 0.0)
                return carry

            lax.fori_loop(0, tiles, mask_tile, 0)
        for side in range(2):
            send_halo(0, side, k)
        return carry

    lax.fori_loop(0, chunks, mask_chunk, 0)

    for side in range(2):
        @pl.when(present(side))
        def _():
            bit_copy(1 - side).wait_recv()
        for i in range(2):
            def unpack(j, carry, side=side, i=i):
                padded = pl.ds(pl.multiple_of(j * words + PAD, PAD), words)
                bit = jnp.bitwise_and(jnp.right_shift(bits_in[side, i], j), 1)
                solid[side * (depth + 2) + i, padded, :] = bit.astype(jnp.float32)
                return carry

            lax.fori_loop(0, 32, unpack, 0)

    column = lax.broadcasted_iota(jnp.int32, (TILE, cols), 1)

    def inplane(ref, plane, start):
        block = ref[plane, pl.ds(start, TILE + 2 * PAD), :]
        centre = block[PAD:PAD + TILE]
        total = block[PAD - 1:PAD - 1 + TILE] + block[PAD + 1:PAD + 1 + TILE]
        total = total + jnp.where(column == 0, 0.0, pltpu.roll(centre, 1, 1))
        total = total + jnp.where(column == cols - 1, 0.0, pltpu.roll(centre, cols - 1, 1))
        return centre, total

    def centre_of(ref, plane, start):
        return ref[plane, pl.ds(pl.multiple_of(start + PAD, PAD), TILE), :]

    def put(ref, plane, start, value):
        ref[plane, pl.ds(pl.multiple_of(start + PAD, PAD), TILE), :] = value

    def fold(value):
        total = value[0:8]
        for i in range(8, TILE, 8):
            total = total + value[i:i + 8]
        return total

    none = jnp.zeros((8, cols), jnp.float32)
    steps = rows // TILE

    def inverse(plane, start):
        _, total = inplane(solid, plane + 1, start)
        total = total + centre_of(solid, plane, start) + centre_of(solid, plane + 2, start)
        return 1.0 / jnp.maximum(6.0 - total, 1.0)

    def first(t, rz):
        start = pl.multiple_of(t * TILE, TILE)
        at = pl.ds(start, TILE)
        for plane in range(depth):
            value = jnp.where(flags[plane, at, :] == 1, inverse(plane + 1, start), 0.0)
            inv[plane + 1, at, :] = value
            residual = r0[plane, at, :]
            precond = residual * value
            put(u0, plane, start, precond)
            rz = rz + fold(residual * precond)
        for plane in (0, depth + 1):
            inv[plane, at, :] = inverse(plane, start)
        return rz

    rz = lax.fori_loop(0, steps, first, none)

    def local_part(field, scaled, out, plane, start):
        at = pl.ds(start, TILE)
        _, total = inplane(field, plane, start)
        if plane > 0:
            total = total + centre_of(field, plane - 1, start)
        if plane < depth - 1:
            total = total + centre_of(field, plane + 1, start)
        image = jnp.where(inv[plane + 1, at, :] > 0.0, scaled[plane, at, :] - total, 0.0)
        out[plane, at, :] = image
        return image

    def second(t, inner):
        start = pl.multiple_of(t * TILE, TILE)
        for plane in range(depth):
            image = local_part(u0, r0, w0, plane, start)
            if 0 < plane < depth - 1:
                put(u1, plane, start, image * inv[plane + 1, pl.ds(start, TILE), :])
                inner = inner + fold(image * centre_of(u0, plane, start))
        return inner

    inner = lax.fori_loop(0, steps, second, none)

    def edge_one(side, inner):
        plane = side * (depth - 1)

        def step(k, inner):
            wait_halo(0, side, k)

            def tile(t, inner):
                start = row(k, t)
                at = pl.ds(start, TILE)
                value = inv[plane + 1, at, :]
                beyond = halo_r[side, at, :] * inv[side * (depth + 1), at, :]
                image = jnp.where(value > 0.0, w0[plane, at, :] - beyond, 0.0)
                w0[plane, at, :] = image
                put(u1, plane, start, image * value)
                return inner + fold(image * centre_of(u0, plane, start))

            inner = lax.fori_loop(0, tiles, tile, inner)
            send_halo(1, side, k)
            return inner

        return lax.fori_loop(0, chunks, step, inner)

    inner = edge_one(first_side, inner)
    inner = edge_one(1 - first_side, inner)

    def lanes(value):
        total = value[:, 0:128]
        for i in range(128, cols, 128):
            total = total + value[:, i:i + 128]
        return total

    def near_copy(turn, j):
        return pltpu.make_async_remote_copy(
            src_ref=mine.at[turn, 0],
            dst_ref=near_got.at[turn, low],
            send_sem=near_send.at[turn, j],
            recv_sem=near_recv.at[turn, low],
            device_id=(near_ids[j - 1],),
            device_id_type=MESH,
        )

    def far_copy(turn, j):
        return pltpu.make_async_remote_copy(
            src_ref=mine.at[turn, 1],
            dst_ref=far_got.at[turn, high],
            send_sem=far_send.at[turn, j],
            recv_sem=far_recv.at[turn, high],
            device_id=(far_ids[j - 1],),
            device_id_type=MESH,
        )

    def sum_start(turn, one, two):
        mine[turn, 0, 0] = lanes(one)
        mine[turn, 0, 1] = lanes(two)
        for j in range(1, near):
            near_copy(turn, j).start()

    def arrived(turn, got, slot, send, recv, other):
        return pltpu.make_async_remote_copy(
            src_ref=got.at[turn, slot],
            dst_ref=got.at[turn, slot],
            send_sem=send.at[turn, 0],
            recv_sem=recv.at[turn, slot],
            device_id=(other,),
            device_id_type=MESH,
        )

    def sum_middle(turn):
        near_got[turn, low] = mine[turn, 0]
        for j in range(1, near):
            slot = lax.rem(low + j, near)
            arrived(turn, near_got, slot, near_send, near_recv, near_ids[j - 1]).wait_recv()
        total = near_got[turn, 0]
        for i in range(1, near):
            total = total + near_got[turn, i]
        mine[turn, 1] = total
        for j in range(1, far):
            far_copy(turn, j).start()

    def sum_end(turn):
        far_got[turn, high] = mine[turn, 1]
        for j in range(1, far):
            slot = lax.rem(high + j, far)
            arrived(turn, far_got, slot, far_send, far_recv, far_ids[j - 1]).wait_recv()
        total = far_got[turn, 0]
        for i in range(1, far):
            total = total + far_got[turn, i]
        return (
            jnp.sum(total[0], keepdims=True),
            jnp.sum(total[1], keepdims=True),
        )

    sum_start(0, rz, inner)

    def third(t, carry):
        start = pl.multiple_of(t * TILE, TILE)
        for plane in range(depth):
            local_part(u1, w0, w1, plane, start)
        return carry

    half = steps // 2
    lax.fori_loop(0, half, third, 0)
    sum_middle(0)
    lax.fori_loop(half, steps, third, 0)
    rz_old, product = sum_end(0)
    step_old = rz_old / product

    def contribution(plane, start, image, carry):
        at = pl.ds(start, TILE)
        along = w0[plane, at, :]
        residual = r0[plane, at, :] - step_old * along
        precond = centre_of(u0, plane, start) - step_old * centre_of(u1, plane, start)
        applied = along - step_old * image
        return (
            carry[0] + fold(residual * precond),
            carry[1] + fold(applied * precond),
        )

    carry = (none, none)
    for plane in range(1, depth - 1):
        def whole(t, carry, plane=plane):
            start = pl.multiple_of(t * TILE, TILE)
            return contribution(plane, start, w1[plane, pl.ds(start, TILE), :], carry)

        carry = lax.fori_loop(0, steps, whole, carry)

    def edge_two(side, carry):
        plane = side * (depth - 1)

        def step(k, carry):
            wait_halo(1, side, k)

            def tile(t, carry):
                start = row(k, t)
                at = pl.ds(start, TILE)
                image = w1[plane, at, :] - halo_u[side, at, :]
                image = jnp.where(inv[plane + 1, at, :] > 0.0, image, 0.0)
                w1[plane, at, :] = image
                return contribution(plane, start, image, carry)

            return lax.fori_loop(0, tiles, tile, carry)

        return lax.fori_loop(0, chunks, step, carry)

    carry = edge_two(first_side, carry)
    carry = edge_two(1 - first_side, carry)
    sum_start(1, *carry)
    sum_middle(1)
    rz_now, product = sum_end(1)
    blend = rz_now / rz_old
    step_size = rz_now / (product - blend * rz_now / step_old)

    def stores(plane, k):
        at = pl.ds(pl.multiple_of(k * chunk, chunk), chunk)
        return (
            pltpu.make_async_copy(rhs.at[plane, at], sol_hbm.at[plane, at], out_sem.at[0, plane, k]),
            pltpu.make_async_copy(w1.at[plane, at], res_hbm.at[plane, at], out_sem.at[1, plane, k]),
        )

    for plane in range(depth):
        def last(k, carry, plane=plane):
            def tile(t, carry):
                start = row(k, t)
                at = pl.ds(start, TILE)
                direction = centre_of(u0, plane, start)
                along = w0[plane, at, :]
                precond = direction - step_old * centre_of(u1, plane, start)
                applied = along - step_old * w1[plane, at, :]
                residual = r0[plane, at, :] - step_old * along
                rhs[plane, at, :] = step_old * direction + step_size * (precond + blend * direction)
                w1[plane, at, :] = residual - step_size * (applied + blend * along)
                return carry

            lax.fori_loop(0, tiles, tile, 0)
            for copy in stores(plane, k):
                copy.start()
            return carry

        lax.fori_loop(0, chunks, last, 0)

    for side in range(2):
        @pl.when(present(side))
        def _():
            bit_copy(side).wait_send()
            for phase in range(2):
                for k in range(chunks):
                    halo_copy(phase, side, k).wait_send()
    for turn in range(2):
        for j in range(1, near):
            near_copy(turn, j).wait_send()
        for j in range(1, far):
            far_copy(turn, j).wait_send()
    for plane in range(depth):
        for k in range(chunks):
            for copy in stores(plane, k):
                copy.wait()


def body(count, right_side, cell_flags):
    depth, rows, cols = right_side.shape
    near = math.gcd(count, 8)
    far = count // near
    chunk = math.gcd(rows, 64)
    chunks = rows // chunk
    f32 = jnp.float32
    field = pltpu.VMEM((depth, rows, cols), f32)
    padded = pltpu.VMEM((depth, rows + 2 * PAD, cols), f32)
    outer = len({0, 1, depth - 2, depth - 1})
    dma = pltpu.SemaphoreType.DMA
    shape = jax.ShapeDtypeStruct((depth, rows, cols), f32)
    return pl.pallas_call(
        functools.partial(kernel, count, near, chunk),
        out_shape=(shape, shape),
        in_specs=[pl.BlockSpec(memory_space=pl.ANY)] * 2,
        out_specs=(pl.BlockSpec(memory_space=pl.ANY),) * 2,
        scratch_shapes=[
            field,
            pltpu.VMEM((depth, rows, cols), jnp.int32),
            field,
            pltpu.VMEM((depth + 2, rows, cols), f32),
            pltpu.VMEM((depth + 4, rows + 2 * PAD, cols), f32),
            padded, padded, field, field,
            pltpu.VMEM((2, rows, cols), f32),
            pltpu.VMEM((2, rows, cols), f32),
            pltpu.VMEM((outer, rows // 32, cols), jnp.int32),
            pltpu.VMEM((2, 2, rows // 32, cols), jnp.int32),
            pltpu.VMEM((2, 2, 2, 8, 128), f32),
            pltpu.VMEM((2, near, 2, 8, 128), f32),
            pltpu.VMEM((2, far, 2, 8, 128), f32),
            dma((2, depth)),
            dma((2, depth, chunks)),
            dma((2,)), dma((2,)),
            dma((2, 2, chunks)), dma((2, 2, chunks)),
            dma((2, near)), dma((2, near)),
            dma((2, far)), dma((2, far)),
        ],
        compiler_params=pltpu.CompilerParams(
            collective_id=0, has_side_effects=True, vmem_limit_bytes=60 * 2**20
        ),
    )(right_side, cell_flags)


def solution(mesh):
    placed = (P("gz", None, None), P("gz", None, None))
    return jax.shard_map(
        functools.partial(body, mesh.shape["gz"]),
        mesh=mesh,
        in_specs=placed,
        out_specs=placed,
        check_vma=False,
    )
```

```python
import functools
import math

import jax
import jax.numpy as jnp
from jax import lax
from jax.experimental import pallas as pl
from jax.experimental.pallas import tpu as pltpu
from jax.sharding import PartitionSpec as P

MESH = pl.DeviceIdType.MESH
TILE = 16
PAD = 8
AHEAD = 2
VMEM_BYTES = 67_043_328


def kernel(
    count, near, chunk,
    side_hbm, flag_hbm, sol_ref, res_ref,
    rhs, flags, r0, inv, solid, u0, u1, w0, w1, halo_r, halo_u, bits_out, bits_in,
    mine, near_got, far_got,
    in_sem, bit_send, bit_recv, halo_send, halo_recv,
    near_send, near_recv, far_send, far_recv,
):
    depth, rows, cols = rhs.shape
    words = rows // 32
    chunks = rows // chunk
    tiles = chunk // TILE
    far = count // near
    me = lax.axis_index("gz")
    low, high = lax.rem(me, near), me // near
    first_side = 1 - lax.rem(me, 2)

    def load(plane, which):
        source, target = ((flag_hbm, flags), (side_hbm, rhs))[which]
        return pltpu.make_async_copy(source.at[plane], target.at[plane], in_sem.at[which, plane])

    for plane in range(depth):
        for which in range(2):
            load(plane, which).start()

    def present(side):
        return jnp.where(side == 0, me > 0, me < count - 1)

    def neighbour(side):
        return me - 1 + 2 * side

    near_ids = [high * near + lax.rem(low + j, near) for j in range(1, near)]
    far_ids = [lax.rem(high + j, far) * near + low for j in range(1, far)]
    barrier = pltpu.get_barrier_semaphore()
    for other in near_ids + far_ids:
        pl.semaphore_signal(barrier, inc=1, device_id=(other,), device_id_type=MESH)
    outside = (
        jnp.logical_and(low == 0, me > 0),
        jnp.logical_and(low == near - 1, me < count - 1),
    )
    for side in range(2):
        @pl.when(outside[side])
        def _():
            pl.semaphore_signal(barrier, inc=1, device_id=(neighbour(side),), device_id_type=MESH)

    blank = jnp.zeros((PAD, cols), jnp.float32)
    for ref in (u0, u1, solid):
        for plane in range(ref.shape[0]):
            ref[plane, 0:PAD, :] = blank
            ref[plane, rows + PAD:rows + 2 * PAD, :] = blank
    for side in range(2):
        @pl.when(jnp.logical_not(present(side)))
        def _():
            bits_in[side] = jnp.zeros((2, words, cols), jnp.int32)

            def clear(t, carry):
                at = pl.ds(pl.multiple_of(t * TILE, TILE), TILE)
                halo_r[side, at, :] = jnp.zeros((TILE, cols), jnp.float32)
                halo_u[side, at, :] = jnp.zeros((TILE, cols), jnp.float32)
                return carry

            lax.fori_loop(0, rows // TILE, clear, 0)

    def halo_copy(phase, side, k):
        at = pl.multiple_of(k * chunk, chunk)
        plane = side * (depth - 1)
        if phase == 0:
            source, target = r0.at[plane, pl.ds(at, chunk)], halo_r
        else:
            source, target = u1.at[plane, pl.ds(pl.multiple_of(at + PAD, PAD), chunk)], halo_u
        return pltpu.make_async_remote_copy(
            src_ref=source,
            dst_ref=target.at[1 - side, pl.ds(at, chunk)],
            send_sem=halo_send.at[phase, side, k],
            recv_sem=halo_recv.at[phase, 1 - side, k],
            device_id=(neighbour(side),),
            device_id_type=MESH,
        )

    def halo_arrival(phase, side, k):
        at = pl.multiple_of(k * chunk, chunk)
        target = halo_r if phase == 0 else halo_u
        return pltpu.make_async_remote_copy(
            src_ref=target.at[side, pl.ds(at, chunk)],
            dst_ref=target.at[side, pl.ds(at, chunk)],
            send_sem=halo_send.at[phase, side, k],
            recv_sem=halo_recv.at[phase, side, k],
            device_id=(neighbour(side),),
            device_id_type=MESH,
        )

    def send_halo(phase, side, k):
        @pl.when(present(side))
        def _():
            halo_copy(phase, side, k).start()

    def wait_halo(phase, side, k):
        @pl.when(present(side))
        def _():
            halo_arrival(phase, side, k).wait_recv()

    def row(k, t):
        return pl.multiple_of(k * chunk + t * TILE, TILE)

    for plane in range(depth):
        load(plane, 0).wait()
        load(plane, 1).wait()
    edge_first = [0, depth - 1] + list(range(1, depth - 1))

    def mask_rows(k):
        for plane in edge_first:
            def mask_tile(t, carry, plane=plane):
                at = pl.ds(row(k, t), TILE)
                r0[plane, at, :] = jnp.where(flags[plane, at, :] == 1, rhs[plane, at, :], 0.0)
                return carry

            lax.fori_loop(0, tiles, mask_tile, 0)

    def send_both(phase, k):
        for side in range(2):
            send_halo(phase, side, k)

    def mask_chunk(k, carry):
        mask_rows(k)
        send_both(0, k)
        return carry

    mask_rows(0)
    peers = near + far - 2 + outside[0].astype(jnp.int32) + outside[1].astype(jnp.int32)
    pl.semaphore_wait(barrier, peers)

    send_both(0, 0)

    outer = sorted({0, 1, depth - 2, depth - 1})
    for plane in range(depth):

        def pack(j, word, plane=plane):
            at = pl.ds(pl.multiple_of(j * words, words), words)
            is_solid = flags[plane, at, :] == 2
            padded = pl.ds(pl.multiple_of(j * words + PAD, PAD), words)
            solid[plane + 2, padded, :] = jnp.where(is_solid, 1.0, 0.0)
            return word | jnp.left_shift(jnp.where(is_solid, 1, 0), j)

        word = lax.fori_loop(0, 32, pack, jnp.zeros((words, cols), jnp.int32))
        if plane in outer:
            bits_out[outer.index(plane)] = word

    def bit_copy(side):
        lead = 0 if side == 0 else len(outer) - 2
        return pltpu.make_async_remote_copy(
            src_ref=bits_out.at[pl.ds(lead, 2)],
            dst_ref=bits_in.at[1 - side],
            send_sem=bit_send.at[side],
            recv_sem=bit_recv.at[1 - side],
            device_id=(neighbour(side),),
            device_id_type=MESH,
        )

    for side in range(2):
        @pl.when(present(side))
        def _():
            bit_copy(side).start()

    lax.fori_loop(1, chunks, mask_chunk, 0)

    for side in range(2):
        @pl.when(present(side))
        def _():
            bit_copy(1 - side).wait_recv()
        for i in range(2):
            def unpack(j, carry, side=side, i=i):
                padded = pl.ds(pl.multiple_of(j * words + PAD, PAD), words)
                bit = jnp.bitwise_and(jnp.right_shift(bits_in[side, i], j), 1)
                solid[side * (depth + 2) + i, padded, :] = bit.astype(jnp.float32)
                return carry

            lax.fori_loop(0, 32, unpack, 0)

    column = lax.broadcasted_iota(jnp.int32, (TILE, cols), 1)

    def inplane(ref, plane, start):
        block = ref[plane, pl.ds(start, TILE + 2 * PAD), :]
        centre = block[PAD:PAD + TILE]
        total = block[PAD - 1:PAD - 1 + TILE] + block[PAD + 1:PAD + 1 + TILE]
        total = total + jnp.where(column == 0, 0.0, pltpu.roll(centre, 1, 1))
        total = total + jnp.where(column == cols - 1, 0.0, pltpu.roll(centre, cols - 1, 1))
        return centre, total

    def centre_of(ref, plane, start):
        return ref[plane, pl.ds(pl.multiple_of(start + PAD, PAD), TILE), :]

    def put(ref, plane, start, value):
        ref[plane, pl.ds(pl.multiple_of(start + PAD, PAD), TILE), :] = value

    def fold(value):
        total = value[0:8]
        for i in range(8, TILE, 8):
            total = total + value[i:i + 8]
        return total

    none = jnp.zeros((8, cols), jnp.float32)
    steps = rows // TILE

    def inverse(plane, start):
        _, total = inplane(solid, plane + 1, start)
        total = total + centre_of(solid, plane, start) + centre_of(solid, plane + 2, start)
        return 1.0 / jnp.maximum(6.0 - total, 1.0)

    def first(t, rz):
        start = pl.multiple_of(t * TILE, TILE)
        at = pl.ds(start, TILE)
        for plane in range(depth):
            value = jnp.where(flags[plane, at, :] == 1, inverse(plane + 1, start), 0.0)
            inv[plane + 1, at, :] = value
            residual = r0[plane, at, :]
            precond = residual * value
            put(u0, plane, start, precond)
            rz = rz + fold(residual * precond)
        for plane in (0, depth + 1):
            inv[plane, at, :] = inverse(plane, start)
        return rz

    rz = lax.fori_loop(0, steps, first, none)

    def local_part(field, scaled, out, plane, start):
        at = pl.ds(start, TILE)
        _, total = inplane(field, plane, start)
        if plane > 0:
            total = total + centre_of(field, plane - 1, start)
        if plane < depth - 1:
            total = total + centre_of(field, plane + 1, start)
        image = jnp.where(inv[plane + 1, at, :] > 0.0, scaled[plane, at, :] - total, 0.0)
        out[plane, at, :] = image
        return image

    def second(t, inner):
        start = pl.multiple_of(t * TILE, TILE)
        for plane in range(depth):
            image = local_part(u0, r0, w0, plane, start)
            if 0 < plane < depth - 1:
                put(u1, plane, start, image * inv[plane + 1, pl.ds(start, TILE), :])
                inner = inner + fold(image * centre_of(u0, plane, start))
        return inner

    inner = lax.fori_loop(0, steps, second, none)

    def edge_one(side, inner, ahead):
        plane = side * (depth - 1)

        def step(k, inner):
            wait_halo(0, side, k)

            def tile(t, inner):
                start = row(k, t)
                at = pl.ds(start, TILE)
                value = inv[plane + 1, at, :]
                beyond = halo_r[side, at, :] * inv[side * (depth + 1), at, :]
                image = jnp.where(value > 0.0, w0[plane, at, :] - beyond, 0.0)
                w0[plane, at, :] = image
                put(u1, plane, start, image * value)
                return inner + fold(image * centre_of(u0, plane, start))

            inner = lax.fori_loop(0, tiles, tile, inner)

            @pl.when(k < ahead)
            def _():
                send_halo(1, side, k)

            return inner

        return lax.fori_loop(0, chunks, step, inner)

    inner = edge_one(first_side, inner, chunks)
    inner = edge_one(1 - first_side, inner, AHEAD)

    def lanes(value):
        total = value[:, 0:128]
        for i in range(128, cols, 128):
            total = total + value[:, i:i + 128]
        return total

    def near_copy(turn, j):
        return pltpu.make_async_remote_copy(
            src_ref=mine.at[turn, 0],
            dst_ref=near_got.at[turn, low],
            send_sem=near_send.at[turn, j],
            recv_sem=near_recv.at[turn, low],
            device_id=(near_ids[j - 1],),
            device_id_type=MESH,
        )

    def far_copy(turn, j):
        return pltpu.make_async_remote_copy(
            src_ref=mine.at[turn, 1],
            dst_ref=far_got.at[turn, high],
            send_sem=far_send.at[turn, j],
            recv_sem=far_recv.at[turn, high],
            device_id=(far_ids[j - 1],),
            device_id_type=MESH,
        )

    def sum_start(turn, one, two):
        mine[turn, 0, 0] = lanes(one)
        mine[turn, 0, 1] = lanes(two)
        for j in range(1, near):
            near_copy(turn, j).start()

    def arrived(turn, got, slot, send, recv, other):
        return pltpu.make_async_remote_copy(
            src_ref=got.at[turn, slot],
            dst_ref=got.at[turn, slot],
            send_sem=send.at[turn, 0],
            recv_sem=recv.at[turn, slot],
            device_id=(other,),
            device_id_type=MESH,
        )

    def sum_middle(turn):
        near_got[turn, low] = mine[turn, 0]
        for j in range(1, near):
            slot = lax.rem(low + j, near)
            arrived(turn, near_got, slot, near_send, near_recv, near_ids[j - 1]).wait_recv()
        total = near_got[turn, 0]
        for i in range(1, near):
            total = total + near_got[turn, i]
        mine[turn, 1] = total
        for j in range(1, far):
            far_copy(turn, j).start()

    def sum_end(turn):
        far_got[turn, high] = mine[turn, 1]
        for j in range(1, far):
            slot = lax.rem(high + j, far)
            arrived(turn, far_got, slot, far_send, far_recv, far_ids[j - 1]).wait_recv()
        total = far_got[turn, 0]
        for i in range(1, far):
            total = total + far_got[turn, i]
        return (
            jnp.sum(total[0], keepdims=True),
            jnp.sum(total[1], keepdims=True),
        )

    sum_start(0, rz, inner)

    def send_rest(k, carry):
        send_halo(1, 1 - first_side, k)
        return carry

    lax.fori_loop(AHEAD, chunks, send_rest, 0)

    def third(t, carry):
        start = pl.multiple_of(t * TILE, TILE)
        for plane in range(depth):
            local_part(u1, w0, w1, plane, start)
        return carry

    half = steps // 2
    lax.fori_loop(0, half, third, 0)
    sum_middle(0)
    lax.fori_loop(half, steps, third, 0)
    rz_old, product = sum_end(0)
    step_old = rz_old / product

    def contribution(plane, start, image, carry):
        at = pl.ds(start, TILE)
        along = w0[plane, at, :]
        residual = r0[plane, at, :] - step_old * along
        precond = centre_of(u0, plane, start) - step_old * centre_of(u1, plane, start)
        applied = along - step_old * image
        return (
            carry[0] + fold(residual * precond),
            carry[1] + fold(applied * precond),
        )

    carry = (none, none)
    for plane in range(1, depth - 1):
        def whole(t, carry, plane=plane):
            start = pl.multiple_of(t * TILE, TILE)
            return contribution(plane, start, w1[plane, pl.ds(start, TILE), :], carry)

        carry = lax.fori_loop(0, steps, whole, carry)

    def edge_two(side, carry):
        plane = side * (depth - 1)

        def step(k, carry):
            wait_halo(1, side, k)

            def tile(t, carry):
                start = row(k, t)
                at = pl.ds(start, TILE)
                image = w1[plane, at, :] - halo_u[side, at, :]
                image = jnp.where(inv[plane + 1, at, :] > 0.0, image, 0.0)
                w1[plane, at, :] = image
                return contribution(plane, start, image, carry)

            return lax.fori_loop(0, tiles, tile, carry)

        return lax.fori_loop(0, chunks, step, carry)

    carry = edge_two(first_side, carry)
    carry = edge_two(1 - first_side, carry)
    sum_start(1, *carry)
    sum_middle(1)
    rz_now, product = sum_end(1)
    blend = rz_now / rz_old
    step_size = rz_now / (product - blend * rz_now / step_old)

    for plane in range(depth):
        def last(t, carry, plane=plane):
            start = pl.multiple_of(t * TILE, TILE)
            at = pl.ds(start, TILE)
            direction = centre_of(u0, plane, start)
            along = w0[plane, at, :]
            precond = direction - step_old * centre_of(u1, plane, start)
            applied = along - step_old * w1[plane, at, :]
            residual = r0[plane, at, :] - step_old * along
            sol_ref[plane, at, :] = step_old * direction + step_size * (precond + blend * direction)
            res_ref[plane, at, :] = residual - step_size * (applied + blend * along)
            return carry

        lax.fori_loop(0, steps, last, 0)

    for side in range(2):
        @pl.when(present(side))
        def _():
            bit_copy(side).wait_send()
            for phase in range(2):
                for k in range(chunks):
                    halo_copy(phase, side, k).wait_send()
    for turn in range(2):
        for j in range(1, near):
            near_copy(turn, j).wait_send()
        for j in range(1, far):
            far_copy(turn, j).wait_send()


def body(count, right_side, cell_flags):
    depth, rows, cols = right_side.shape
    near = math.gcd(count, 8)
    far = count // near
    chunk = math.gcd(rows, 64)
    chunks = rows // chunk
    f32 = jnp.float32
    field = pltpu.VMEM((depth, rows, cols), f32)
    padded = pltpu.VMEM((depth, rows + 2 * PAD, cols), f32)
    outer = len({0, 1, depth - 2, depth - 1})
    dma = pltpu.SemaphoreType.DMA
    grant = VMEM_BYTES - 8 * right_side.size - 2**19
    return pl.pallas_call(
        functools.partial(kernel, count, near, chunk),
        out_shape=(field, field),
        in_specs=[pl.BlockSpec(memory_space=pltpu.HBM)] * 2,
        out_specs=(pl.BlockSpec(memory_space=pltpu.VMEM),) * 2,
        scratch_shapes=[
            field,
            pltpu.VMEM((depth, rows, cols), jnp.int32),
            field,
            pltpu.VMEM((depth + 2, rows, cols), f32),
            pltpu.VMEM((depth + 4, rows + 2 * PAD, cols), f32),
            padded, padded, field, field,
            pltpu.VMEM((2, rows, cols), f32),
            pltpu.VMEM((2, rows, cols), f32),
            pltpu.VMEM((outer, rows // 32, cols), jnp.int32),
            pltpu.VMEM((2, 2, rows // 32, cols), jnp.int32),
            pltpu.VMEM((2, 2, 2, 8, 128), f32),
            pltpu.VMEM((2, near, 2, 8, 128), f32),
            pltpu.VMEM((2, far, 2, 8, 128), f32),
            dma((2, depth)),
            dma((2,)), dma((2,)),
            dma((2, 2, chunks)), dma((2, 2, chunks)),
            dma((2, near)), dma((2, near)),
            dma((2, far)), dma((2, far)),
        ],
        compiler_params=pltpu.CompilerParams(
            collective_id=0, has_side_effects=True, vmem_limit_bytes=grant
        ),
    )(right_side, cell_flags)


def solution(mesh):
    placed = (P("gz", None, None), P("gz", None, None))
    return jax.shard_map(
        functools.partial(body, mesh.shape["gz"]),
        mesh=mesh,
        in_specs=placed,
        out_specs=placed,
        check_vma=False,
    )
```
